256 devices in a mesh: ga: 4 (over x, y), col: 64 (over z, core).
Axes of the slice: x: 2, y: 2, z: 32, core: 2. Of those that a mesh axis runs over, the one named last changes fastest.
The devices are a block of a 4x8x32 slice.
Arguments:
- queries: bfloat16 [2048, 32, 128], P(('ga', 'col')), parts along dimension 0, may hold values from -6 to 6
- patches: bfloat16 [512, 16, 64, 128], P(('ga', 'col')), parts along dimension 0, may hold values from -0.5 to 0.5
- top_ids: int32 [2048, 50], P(('ga', 'col')), parts along dimension 0, may hold values from 0 to 127, all different within a row
Outputs:
- scores: float32 [2048, 128], P('ga', 'col'), parts along dimension 0
- top_scores: float32 [2048, 50], P(('ga', 'col')), parts along dimension 0
The draws below stay inside these ranges and needn't reach their ends.
There are 4 independent parts, one for each index of `ga`. The reference program is written for one: setup_inputs(seed, part) draws one part's arguments, and reference() takes and returns one part's arrays. A program takes and returns all parts, laid end to end along the dimension named above; each array names one. Nothing has to cross between parts.
Inputs may be any that keep to these rules, and one draw needn't show every extreme that they name: `top_ids`: each row names 50 different clips.
All inputs are finite; a program needn't handle non-finite values.
Results may differ from the reference program's by a relative error of at most 0.0003.
Values may be sent and summed in bfloat16 or wider, within the bound.
No kernel may reach another device: no remote copies, remote signals or barrier semaphores. Data moves between devices by JAX's collectives and lax.ppermute only.
A program may use at most 64 MiB of HBM per device.

```python
import jax
import jax.numpy as jnp
from jax import lax

D = 128
L = 32
F = 16
P_SIZE = 64
Q = 512
CLIPS = 128
K = 50


def block_scale(stream_key, shape, split, smallest, largest):
    factor_of, own = 1.0, jax.random.fold_in(stream_key, 6)
    for dim, parts in split:
        draws = jnp.exp(jax.random.uniform(jax.random.fold_in(own, dim), (parts,), jnp.float32, smallest / len(split), largest / len(split)))
        factor_of = factor_of * jnp.repeat(draws, shape[dim] // parts).reshape([-1 if axis == dim else 1 for axis in range(len(shape))])
    return factor_of


def different_ones(stream_key, rows, count, top, lift):
    ranking = jax.random.permutation(jax.random.fold_in(stream_key, 1), count)
    favour = ranking
    for power in range(3):
        favour = favour * favour // count
    favour = favour * lift // count
    chance = jax.random.randint(jax.random.fold_in(stream_key, 2), (rows, count), 0, 4096) + favour
    sure = jax.random.permutation(jax.random.fold_in(stream_key, 3), rows)[jnp.arange(count) % rows]
    chance = jnp.where(jnp.arange(rows)[:, None] == sure[None, :], 1 << 14, chance)
    priority = chance * count + jnp.arange(count)
    return lax.top_k(priority.astype(jnp.int32), top)[1].astype(jnp.int32)


def centred(own_key, dims, spread, reach, split=(), kind=jnp.bfloat16):
    drawn = spread * jax.random.normal(own_key, dims, jnp.float32)
    if split:
        drawn = drawn * block_scale(own_key, dims, split, -0.22, 0.18)
    return jnp.clip(drawn, -reach, reach).astype(kind)


def setup_inputs(seed: int = 0, part: int = 0) -> dict:
    splits = jax.random.split(jax.random.key(seed), 4)
    own_keys = jax.random.split(jax.random.fold_in(splits[3], part), 4)
    queries = centred(own_keys[0], (Q, L, D), 1.0, 6.0, ((0, 64),))
    patches = centred(own_keys[1], (CLIPS, F, P_SIZE, D), D ** -0.5, 0.5, ((0, 64),))
    top_ids = different_ones(own_keys[2], Q, CLIPS, K, 0)
    return {"queries": queries, "patches": patches, "top_ids": top_ids}


def reference(queries, patches, top_ids):
    flat_queries = queries.reshape(-1, D).astype(jnp.float32)

    def one_clip(clip):
        block = clip.reshape(-1, D).astype(jnp.float32)
        sim = jnp.dot(flat_queries, block.T, precision=lax.Precision.HIGHEST, preferred_element_type=jnp.float32)
        best = jnp.max(sim, axis=1).reshape(Q, L)
        return jnp.sum(best, axis=1) / L

    scores = lax.map(one_clip, patches).T
    top_scores = jnp.take_along_axis(scores, top_ids, axis=1)
    return scores, top_scores
```

```python
import jax
import jax.numpy as jnp
from jax import lax
from jax.sharding import PartitionSpec as P


CORES = 2


def solution(mesh):
    devices = mesh.shape["col"]
    chips = devices // CORES
    steps = chips // 4
    same_core = [list(range(core, devices, CORES)) for core in range(CORES)]

    def hop(x, distance):
        step = CORES * distance
        return lax.ppermute(x, "col", [(i, (i + step) % devices) for i in range(devices)])

    def partner(x):
        return lax.ppermute(x, "col", [(i, i ^ 1) for i in range(devices)])

    def per_device(queries, patches, top_ids):
        mine, tokens, width = queries.shape
        clip_count, frames, per_frame, _ = patches.shape
        rows = mine * tokens
        flat = patches.reshape(clip_count, frames * per_frame, width)
        chip = lax.axis_index("col") // CORES
        core = lax.axis_index("col") % CORES

        right = left = queries.reshape(rows, width)
        best = [None] * steps
        blocks = []
        ties = {3: (0, 1), 4: (2, 3), 5: (4,), 6: (5,), 7: (6,)}
        clips = None

        def score(block):
            sim = lax.dot_general(block, clips, (((1,), (2,)), ((), ())), preferred_element_type=jnp.float32)
            return jnp.max(sim, axis=2)

        for s in range(steps):
            right, left = hop(right, 2 if s else 1), hop(left, -2 if s else -1)
            blocks.append(jnp.concatenate([right, left], 0))
            if s == 0:
                ahead = hop(flat[0:1], -1)
                behind = hop(flat[1:2], 1)
                own = jnp.concatenate([flat, ahead, behind], 0)
                clips = jnp.concatenate([own, partner(own)], 0)
            if s in ties and s + 1 < steps:
                done = [score(blocks[b]) for b in ties[s]]
                right, left, *done = lax.optimization_barrier((right, left, *done))
                for b, x in zip(ties[s], done):
                    best[b] = x
        for b in range(steps):
            if best[b] is None:
                best[b] = score(blocks[b])
        best = jnp.stack(best).reshape(2 * steps, mine, tokens, -1)
        part = jnp.sum(best, axis=2) / tokens
        cols = part.transpose(0, 2, 1).reshape(2 * steps, -1)
        owner = lax.broadcasted_iota(jnp.int32, (chips, 1), 0)
        table = jnp.zeros((chips, cols.shape[1]), jnp.float32)
        for s in range(steps):
            for k, sign in ((0, 1), (1, -1)):
                src = (chip - sign * (1 + 2 * s)) % chips
                table = jnp.where(owner == src, cols[2 * s + k][None], table)
        got = lax.all_to_all(
            table, "col", split_axis=0, concat_axis=0, tiled=True, axis_index_groups=same_core
        )
        got = got.reshape(chips, CORES, 2 * clip_count, mine)
        table = table.reshape(chips, CORES, 2 * clip_count, mine)
        other = partner(table[:, 1])
        lo = jnp.where(core == 0, table[:, 0], other)
        hi = jnp.where(core == 0, other, table[:, 0])
        both = jnp.stack([lo, hi], 1)
        first = both[:, :, 0] + hop(both[:, :, 2], 1)
        second = both[:, :, 1] + hop(both[:, :, 3], -1)
        scores = jnp.stack([first, second], 3).reshape(chips * CORES * mine, clip_count)
        lo = jnp.where(core == 0, got[:, 0], got[:, 1])
        hi = jnp.where(core == 0, got[:, 1], got[:, 0])
        got = jnp.stack([lo, hi], 1)
        first = got[:, :, 0] + jnp.roll(got[:, :, 2], 1, axis=0)
        second = got[:, :, 1] + jnp.roll(got[:, :, 3], -1, axis=0)
        full = jnp.stack([first, second], 2).reshape(chips * CORES * clip_count, mine)
        clip = lax.broadcasted_iota(jnp.int32, (1, 1, full.shape[0]), 2)
        top = jnp.sum(jnp.where(top_ids[:, :, None] == clip, full.T[:, None, :], 0.0), axis=2)
        return scores, top

    return jax.shard_map(
        per_device,
        mesh=mesh,
        in_specs=(
            P(("ga", "col"), None, None),
            P(("ga", "col"), None, None, None),
            P(("ga", "col"), None),
        ),
        out_specs=(P("ga", "col"), P(("ga", "col"), None)),
        check_vma=False,
    )
```

```python
import jax
import jax.numpy as jnp
from jax import lax
from jax.sharding import PartitionSpec as P


CORES = 2


def solution(mesh):
    devices = mesh.shape["col"]
    chips = devices // CORES
    steps = chips // 4
    same_core = [list(range(core, devices, CORES)) for core in range(CORES)]

    def hop(x, distance):
        step = CORES * distance
        return lax.ppermute(x, "col", [(i, (i + step) % devices) for i in range(devices)])

    def partner(x):
        return lax.ppermute(x, "col", [(i, i ^ 1) for i in range(devices)])

    def per_device(queries, patches, top_ids):
        mine, tokens, width = queries.shape
        clip_count, frames, per_frame, _ = patches.shape
        rows = mine * tokens
        flat = patches.reshape(clip_count, frames * per_frame, width)
        chip = lax.axis_index("col") // CORES
        core = lax.axis_index("col") % CORES

        right = left = queries.reshape(rows, width)
        rights, lefts = [], []
        best = []
        ties = {3: (0, 1), 4: (2, 3), 5: (4,), 6: (5,), 7: (6,)}
        clips = None

        def score(*parts):
            block = jnp.concatenate(parts, 0) if len(parts) > 1 else parts[0]
            sim = lax.dot_general(block, clips, (((1,), (2,)), ((), ())), preferred_element_type=jnp.float32)
            return jnp.max(sim, axis=2)

        for s in range(steps):
            right = hop(right, 2 if s else 1)
            left = hop(left, -2 if s else -1)
            rights.append(right)
            lefts.append(left)
            if s == 0:
                ahead = hop(flat[0:1], -1)
                behind = hop(flat[1:2], 1)
                own = jnp.concatenate([flat, ahead, behind], 0)
                clips = jnp.concatenate([own, partner(own)], 0)
            if s in ties:
                done = score(*[x for b in ties[s] for x in (rights[b], lefts[b])])
                right, done = lax.optimization_barrier((right, done))
                best.append(done)
        best += [score(right), score(left)]
        part = jnp.concatenate(best, 0).reshape(steps, 2, mine, tokens, -1)
        part = jnp.sum(part, axis=3) / tokens
        part = jnp.concatenate([part[:, 1], part[::-1, 0]], 0).transpose(0, 2, 1)
        ahead_of = jnp.stack([jnp.zeros_like(part), part], 1).reshape(chips, *part.shape[1:])
        table = lax.dynamic_slice_in_dim(jnp.concatenate([ahead_of, ahead_of], 0), chips - chip, chips, 0)
        got = lax.all_to_all(
            table.reshape(chips, 1, -1), "col", split_axis=0, concat_axis=0, tiled=True, axis_index_groups=same_core
        )
        held = 2 * clip_count
        other = partner(table[:, held:])
        both = jnp.stack([table[:, :held], other])
        first = both[:, :, 0] + hop(both[:, :, 2], 1)
        second = both[:, :, 1] + hop(both[:, :, 3], -1)
        both = jnp.stack([first, second])
        both = jnp.where(core == 0, both, both[:, ::-1])
        scores = both.transpose(0, 2, 1, 3).reshape(clip_count, -1).T
        got = got.reshape(-1, mine)
        slot = lax.broadcasted_iota(jnp.int32, (1, 1, got.shape[0]), 2)
        kind = slot % held
        where = slot // (2 * held) + jnp.where(kind == 2, 1, 0) - jnp.where(kind == 3, 1, 0)
        clip_core = (slot // held + core) % CORES
        ident = ((where + chips) % chips * CORES + clip_core) * clip_count + kind % clip_count
        top = jnp.sum(jnp.where(top_ids[:, :, None] == ident, got.T[:, None, :], 0.0), axis=2)
        return scores, top

    return jax.shard_map(
        per_device,
        mesh=mesh,
        in_specs=(
            P(("ga", "col"), None, None),
            P(("ga", "col"), None, None, None),
            P(("ga", "col"), None),
        ),
        out_specs=(P("ga", "col"), P(("ga", "col"), None)),
        check_vma=False,
    )
```
